32 devices in a mesh: plane: 4 (over y, core), line: 8 (over z, x).
Axes of the slice: x: 2, y: 2, z: 4, core: 2. Of those that a mesh axis runs over, the one named last changes fastest.
Arguments:
- flow_state: float32 [5, 64, 1024, 128], P(None, 'plane', 'line'), may hold values from -6 to 6
- wave_speed: float32 [64, 1024, 128], P('plane', 'line'), may hold values from 0.3 to 3
- left_eig: float32 [5, 5], replicated, may hold values from -2.5 to 2.5
- right_eig: float32 [5, 5], replicated, may hold values from -2.5 to 2.5
- lower_inverse: float32 [5, 64, 1024, 128], P(None, 'plane', 'line')
- upper_inverse: float32 [5, 64, 1024, 128], P(None, 'plane', 'line')
- lower_link: float32 [3, 5, 64, 8, 128], P(None, None, 'plane', 'line'), may hold values from 0.29 to 0.33
- upper_link: float32 [3, 5, 64, 8, 128], P(None, None, 'plane', 'line'), may hold values from 0.29 to 0.33
- donor_rows: int32 [4, 8, 4, 32], P('plane', 'line'), may hold values from 0 to 1919
- stencil_offsets: int32 [4, 8, 4, 32], P('plane', 'line'), may hold values from 1 to 128, as said below
- donor_weights: float32 [2, 4, 8, 4, 32], P(None, 'plane', 'line'), may hold values from 0.2 to 0.8
- block_counts: int32 [4, 8, 4], P(None, 'line', 'plane'), may hold values from 8 to 32, as said below
- receptor_rows: int32 [4, 8, 4, 32], P('plane', 'line'), may hold values from 0 to 2047, as said below
Outputs:
- next_state: float32 [5, 64, 1024, 128], P(None, 'plane', 'line')
The draws below stay inside these ranges and needn't reach their ends.
Inputs may be any that keep to these rules, and one draw needn't show every extreme that they name: `donor_rows`: a donor row leaves room for the stencil offset inside its block. `stencil_offsets`: each offset is 1 or 128. `block_counts`: at most 32 blocks from one source block to one owner; in every line block one owner receives 32 from every source. `receptor_rows`: on each receptor block the rows of all sources and slots are distinct.
All inputs are finite; a program needn't handle non-finite values.
Results may differ from the reference program's by a relative error of at most 0.00014.
Values sent between devices are 32-bit elements; how exact they have to be, the bound alone decides.
A program may use at most 128 MiB of HBM per device.

```python
import math
import jax
import jax.numpy as jnp
from jax import lax

FLOW_VARIABLES = 5
R = 128
PL_DEV = 16
LDEV = 128
CAP = 32
NPL = 64
NL = 1024
N_PLANE = 4
N_LINE = 8


def band_inverse(key, reflect):
    random_keys = jax.random.split(key, 8)
    lines = N_LINE * LDEV
    plane_list = N_PLANE * PL_DEV
    row_pos = (jnp.arange(lines, dtype=jnp.int32) % LDEV)[None, None, :, None]
    col_pos = jnp.arange(LDEV, dtype=jnp.int32)[None, None, None, :]
    if reflect:
        row_pos = LDEV - 1 - row_pos
        col_pos = LDEV - 1 - col_pos
    shape_all = (FLOW_VARIABLES, plane_list, lines, LDEV)
    spread_part = jax.random.normal(random_keys[0], shape_all, jnp.float32) * 0.4 / jnp.sqrt(row_pos.astype(jnp.float32) + 1.0)
    diagonal = jax.random.uniform(random_keys[1], (FLOW_VARIABLES, plane_list, lines, 1), jnp.float32, 1.0, 1.5)
    slow_share = 0.5
    sluggish_factor = jax.random.uniform(random_keys[2], (FLOW_VARIABLES, plane_list, 1, 1, 1), jnp.float32) < slow_share
    sluggish_retained = jax.random.uniform(random_keys[4], (FLOW_VARIABLES, plane_list, N_LINE, 1, 1), jnp.float32, 0.95, 1.0)
    quick_retained = jnp.exp(jax.random.uniform(random_keys[5], (FLOW_VARIABLES, plane_list, N_LINE, 1, 1), jnp.float32, math.log(0.05), math.log(0.3)))
    sudden_jump = jax.random.uniform(random_keys[6], (FLOW_VARIABLES, plane_list, N_LINE, 1, 1), jnp.float32) < 1.0 / N_LINE
    jump_threshold = jax.random.uniform(random_keys[7], (FLOW_VARIABLES, plane_list, N_LINE, 1, 1), jnp.float32, 0.5, 0.8)
    retained_mask = jnp.where(sluggish_factor, sluggish_retained, quick_retained) * jnp.where(sudden_jump, jump_threshold, 1.0)
    retained_mask = jnp.broadcast_to(retained_mask, (FLOW_VARIABLES, plane_list, N_LINE, LDEV, 1)).reshape(FLOW_VARIABLES, plane_list, lines, 1)
    carried = retained_mask * (1.0 + 0.03 * jax.random.normal(random_keys[3], shape_all, jnp.float32))
    below = jnp.where(col_pos < 2, carried, spread_part)
    return jnp.where(col_pos == row_pos, diagonal, jnp.where(col_pos < row_pos, below, 0.0))


def draw_lower_inverse(key, part):
    return band_inverse(jax.random.fold_in(key, 11), False)


def draw_upper_inverse(key, part):
    return band_inverse(jax.random.fold_in(key, 12), True)


def draw_stencil_offsets(key, part):
    picks = jax.random.randint(key, (N_PLANE, N_LINE, N_PLANE, CAP), 0, 2)
    return (1 + (LDEV - 1) * picks).astype(jnp.int32)


def draw_block_counts(key, part):
    random_keys = jax.random.split(jax.random.fold_in(key, 21), 2)
    base = jax.random.randint(random_keys[0], (N_PLANE, N_LINE, N_PLANE), CAP // 4, CAP // 2 + 1)
    hottest = jax.random.randint(random_keys[1], (N_LINE,), 0, N_PLANE)
    owner = jnp.arange(N_PLANE, dtype=jnp.int32)[None, None, :]
    return jnp.where(owner == hottest[None, :, None], CAP, base).astype(jnp.int32)


def first_rows(subkey):
    return jax.random.permutation(subkey, PL_DEV * LDEV)[:N_PLANE * CAP]


def draw_receptor_rows(key, part):
    random_keys = jax.random.split(jax.random.fold_in(key, 31), N_PLANE * N_LINE)
    chosen = jax.vmap(first_rows)(random_keys)
    return chosen.reshape(N_PLANE, N_LINE, N_PLANE, CAP).astype(jnp.int32)


def with_ends(result, key, smallest, high):
    longest = result.shape.index(max(result.shape))
    spots = []
    for shift in (0, 1):
        where = [jax.random.randint(jax.random.fold_in(key, axis), (), 0, length) for axis, length in enumerate(result.shape)]
        where[longest] = (where[longest] + shift) % result.shape[longest]
        spots.append(tuple(where))
    return result.at[spots[0]].set(smallest).at[spots[1]].set(high)


def shard_levels(own_key, extent, pieces, smallest, largest):
    def one(dim, shards_of):
        draws = jax.random.uniform(jax.random.fold_in(jax.random.fold_in(own_key, 6), dim), (shards_of,), jnp.float32, smallest / len(pieces), largest / len(pieces))
        return jnp.repeat(jnp.exp(draws), extent[dim] // shards_of).reshape((-1,) + (1,) * (len(extent) - dim - 1))

    gain = one(*pieces[0])
    for cut in pieces[1:]:
        gain = gain * one(*cut)
    return gain


def gaussian(rng, shape, deviation, bound, shards=(), kind=jnp.bfloat16):
    drawn = jax.random.normal(rng, shape, jnp.float32) * deviation
    if len(shards) > 0:
        drawn = shard_levels(rng, shape, shards, -0.22, 0.18) * drawn
    return jnp.clip(drawn, min=-bound, max=bound).astype(kind)


def setup_inputs(seed: int = 0) -> dict:
    arg_keys = jax.random.split(jax.random.key(seed), 14)
    flow_state = gaussian(arg_keys[0], (FLOW_VARIABLES, NPL, NL, R), 1.0, 6.0, ((1, 4), (2, 8)), jnp.float32)
    wave_speed = jnp.clip(jnp.exp(math.log(3.0) - 2.3025851 * jax.random.uniform(arg_keys[1], (NPL, NL, R), jnp.float32) ** shard_levels(arg_keys[1], (NPL, NL, R), ((0, 4), (1, 8)), -0.2, 0.2)), 0.3, 3.0)
    left_eig = gaussian(arg_keys[2], (FLOW_VARIABLES, FLOW_VARIABLES), FLOW_VARIABLES ** -0.5, 2.5, (), jnp.float32)
    right_eig = gaussian(arg_keys[3], (FLOW_VARIABLES, FLOW_VARIABLES), FLOW_VARIABLES ** -0.5, 2.5, (), jnp.float32)
    lower_inverse = draw_lower_inverse(jax.random.fold_in(arg_keys[13], 71), 0)
    upper_inverse = draw_upper_inverse(jax.random.fold_in(arg_keys[13], 71), 0)
    lower_link = jnp.clip(0.29 + 0.04000002 * jax.random.uniform(arg_keys[6], (3, FLOW_VARIABLES, NPL, N_LINE, R), jnp.float32) ** shard_levels(arg_keys[6], (3, FLOW_VARIABLES, NPL, N_LINE, R), ((2, 4), (3, 8)), -0.2, 0.2), 0.29, 0.33)
    upper_link = jnp.clip(0.29 + 0.04000002 * jax.random.uniform(arg_keys[7], (3, FLOW_VARIABLES, NPL, N_LINE, R), jnp.float32) ** shard_levels(arg_keys[7], (3, FLOW_VARIABLES, NPL, N_LINE, R), ((2, 4), (3, 8)), -0.2, 0.2), 0.29, 0.33)
    donor_rows = with_ends(jax.random.randint(arg_keys[8], (N_PLANE, N_LINE, N_PLANE, CAP), 0, (PL_DEV - 1) * LDEV), jax.random.fold_in(arg_keys[8], 1), 0, ((PL_DEV - 1) * LDEV) - 1).astype(jnp.int32)
    stencil_offsets = draw_stencil_offsets(jax.random.fold_in(arg_keys[13], 71), 0)
    donor_weights = jnp.clip(0.2 + 0.6 * jax.random.uniform(arg_keys[10], (2, N_PLANE, N_LINE, N_PLANE, CAP), jnp.float32) ** shard_levels(arg_keys[10], (2, N_PLANE, N_LINE, N_PLANE, CAP), ((1, 4), (2, 8)), -0.2, 0.2), 0.2, 0.8)
    block_counts = draw_block_counts(jax.random.fold_in(arg_keys[13], 71), 0)
    receptor_rows = draw_receptor_rows(jax.random.fold_in(arg_keys[13], 71), 0)
    return dict(flow_state=flow_state, wave_speed=wave_speed, left_eig=left_eig, right_eig=right_eig, lower_inverse=lower_inverse, upper_inverse=upper_inverse, lower_link=lower_link, upper_link=upper_link, donor_rows=donor_rows, stencil_offsets=stencil_offsets, donor_weights=donor_weights, block_counts=block_counts, receptor_rows=receptor_rows)


exact_mode = lax.Precision.HIGHEST


def tendency_of(extended, patched, wave_speed):
    along_line = extended[:, :, 3:-1] - extended[:, :, 1:-3]
    fourth = extended[:, :, 4:] - 4.0 * extended[:, :, 3:-1] + 6.0 * extended[:, :, 2:-2] - 4.0 * extended[:, :, 1:-3] + extended[:, :, :-4]
    widened = jnp.pad(patched, ((0, 0), (0, 0), (0, 0), (1, 1)))
    along_row = widened[..., 2:] - widened[..., :-2]
    return -wave_speed[None] * (0.5 * (along_line + along_row) + 0.0625 * fourth)


def place_rows(block, target, values):
    return block.at[:, target, :].set(values, mode="drop")


def reference(flow_state, wave_speed, left_eig, right_eig, lower_inverse, upper_inverse, lower_link, upper_link, donor_rows, stencil_offsets, donor_weights, block_counts, receptor_rows):
    rows_dev = PL_DEV * LDEV
    slots = N_PLANE * CAP
    plane_list = N_PLANE * PL_DEV
    blocks = flow_state.reshape(FLOW_VARIABLES, N_PLANE, PL_DEV, N_LINE, LDEV, R).transpose(1, 3, 0, 2, 4, 5).reshape(N_PLANE, N_LINE, FLOW_VARIABLES, rows_dev, R)
    shape_all = (N_PLANE, N_LINE, FLOW_VARIABLES, slots, R)
    first = jnp.broadcast_to(donor_rows.reshape(N_PLANE, N_LINE, 1, slots, 1), shape_all).astype(jnp.int32)
    second = jnp.broadcast_to((donor_rows + stencil_offsets).reshape(N_PLANE, N_LINE, 1, slots, 1), shape_all).astype(jnp.int32)
    weight_near = donor_weights[0].reshape(N_PLANE, N_LINE, 1, slots, 1)
    weight_far = donor_weights[1].reshape(N_PLANE, N_LINE, 1, slots, 1)
    donor_values = weight_near * jnp.take_along_axis(blocks, first, axis=3) + weight_far * jnp.take_along_axis(blocks, second, axis=3)
    received = donor_values.reshape(N_PLANE, N_LINE, FLOW_VARIABLES, N_PLANE, CAP, R).transpose(3, 1, 2, 0, 4, 5).reshape(N_PLANE, N_LINE, FLOW_VARIABLES, slots, R)
    counts = jnp.transpose(block_counts, (2, 1, 0))
    valid = jnp.arange(CAP, dtype=jnp.int32)[None, None, None, :] < counts[..., None]
    target = jnp.where(valid, receptor_rows, rows_dev).reshape(N_PLANE, N_LINE, slots).astype(jnp.int32)
    filled = jax.vmap(jax.vmap(place_rows))(blocks, target, received)
    patched = filled.reshape(N_PLANE, N_LINE, FLOW_VARIABLES, PL_DEV, LDEV, R).transpose(2, 0, 3, 1, 4, 5).reshape(FLOW_VARIABLES, plane_list, N_LINE * LDEV, R)
    extended = jnp.pad(patched, ((0, 0), (0, 0), (2, 2), (0, 0)))
    tendency = tendency_of(extended, patched, wave_speed)
    characteristic = jnp.einsum("vu,upnr->vpnr", left_eig, tendency, precision=exact_mode)
    lower_blocks = lower_inverse.reshape(FLOW_VARIABLES, plane_list, N_LINE, LDEV, LDEV)
    particular = jnp.einsum("vpjik,vpjkr->vpjir", lower_blocks, characteristic.reshape(FLOW_VARIABLES, plane_list, N_LINE, LDEV, R), precision=exact_mode)
    last_value = jnp.zeros((FLOW_VARIABLES, plane_list, R), jnp.float32)
    second_value = jnp.zeros((FLOW_VARIABLES, plane_list, R), jnp.float32)
    sweeps = []
    for index in range(N_LINE):
        inverse = lower_blocks[:, :, index]
        coupling = lower_link[:, :, :, index]
        first_term = (coupling[0] * last_value + coupling[1] * second_value)[:, :, None, :]
        second_term = (coupling[2] * last_value)[:, :, None, :]
        solved = particular[:, :, index] - inverse[:, :, :, 0:1] * first_term - inverse[:, :, :, 1:2] * second_term
        last_value = solved[:, :, -1]
        second_value = solved[:, :, -2]
        sweeps.append(solved)
    forward_sweep = jnp.stack(sweeps, axis=2)
    upper_blocks = upper_inverse.reshape(FLOW_VARIABLES, plane_list, N_LINE, LDEV, LDEV)
    projected = jnp.einsum("vpjik,vpjkr->vpjir", upper_blocks, forward_sweep, precision=exact_mode)
    head_value = jnp.zeros((FLOW_VARIABLES, plane_list, R), jnp.float32)
    following_value = jnp.zeros((FLOW_VARIABLES, plane_list, R), jnp.float32)
    results = []
    for index in range(N_LINE - 1, -1, -1):
        inverse = upper_blocks[:, :, index]
        coupling = upper_link[:, :, :, index]
        first_term = (coupling[0] * head_value + coupling[1] * following_value)[:, :, None, :]
        second_term = (coupling[2] * head_value)[:, :, None, :]
        solved = projected[:, :, index] - inverse[:, :, :, -1:] * first_term - inverse[:, :, :, -2:-1] * second_term
        head_value = solved[:, :, 0]
        following_value = solved[:, :, 1]
        results.insert(0, solved)
    backward_sweep = jnp.stack(results, axis=2).reshape(FLOW_VARIABLES, plane_list, N_LINE * LDEV, R)
    change = jnp.einsum("vu,upnr->vpnr", right_eig, backward_sweep, precision=exact_mode)
    return patched + change
```

```python
import functools
import jax
import jax.numpy as jnp
from jax import lax
from jax.experimental import pallas as pl
from jax.experimental.pallas import tpu as pltpu
from jax.sharding import PartitionSpec as P

MESH = pl.DeviceIdType.MESH
F32 = jnp.float32
BF16 = jnp.bfloat16
PAD = 8
SUB = 8


def split(x):
    hi = x.astype(BF16)
    lo = (x - hi.astype(F32)).astype(BF16)
    return hi, lo


def wide(x):
    hi, lo = split(x)
    both = jnp.concatenate([hi, lo], axis=1)
    return jnp.concatenate([both, both], axis=0)


def product(left_pair, x):
    n = x.shape[1]
    full = jnp.dot(left_pair, wide(x), preferred_element_type=F32)
    return full[:, :n] + full[:, n:]


def kernel(
    np_, nl_, flow, wave, lower, upper, left_eig, right_eig, llink, ulink, drows, doffs, dwts, counts, rrows,
    out,
    ext, wbuf, lbuf, ubuf, lsp, usp, char, obuf, lhs, dsend, drecv, rhs, hsend, hrecv, wedge, cfix,
    amine, atheirs, bmine, btheirs, fin, fsend, ubrow, cor, acor, rows,
    lsem, osem, dsend_s, drecv_s, dloc_s, hsend_s, hrecv_s, asend_s, arecv_s, bsend_s, brecv_s, csend_s, crecv_s,
):
    nv, planes, points, width = lower.shape
    chunks = planes // SUB
    cap = drows.shape[3]
    me = lax.axis_index("plane")
    l = lax.axis_index("line")
    z = l // 2
    x = l % 2
    nz = nl_ // 2
    partner = l + 1 - 2 * x

    barrier = pltpu.get_barrier_semaphore()
    own_chip = me // 2
    peers = [((own_chip + 1 + i) % (np_ // 2)) * 2 + c for i in range(np_ // 2 - 1) for c in (0, 1)]
    peers.append(own_chip * 2 + 1 - me % 2)
    for d in peers:
        pl.semaphore_signal(barrier, inc=1, device_id=(d, l), device_id_type=MESH)
    for step in (1, 2):
        @pl.when(l >= step)
        def _():
            pl.semaphore_signal(barrier, inc=1, device_id=(me, l - step), device_id_type=MESH)

        @pl.when(l + step < nl_)
        def _():
            pl.semaphore_signal(barrier, inc=1, device_id=(me, l + step), device_id_type=MESH)

    flow_in = pltpu.make_async_copy(flow, ext.at[:, :, pl.ds(PAD, points), :], lsem.at[0])
    lower_in = pltpu.make_async_copy(lower, lbuf, lsem.at[1])
    upper_in = pltpu.make_async_copy(upper, ubuf, lsem.at[2])
    wave_in = pltpu.make_async_copy(wave, wbuf, lsem.at[3])
    flow_in.start()
    lower_in.start()
    upper_in.start()
    wave_in.start()

    near = jnp.minimum(l, 2) + jnp.minimum(nl_ - 1 - l, 2)
    pl.semaphore_wait(barrier, len(peers) + near)

    flow_in.wait()

    def gather(d):
        def one(c, carry):
            k1 = drows[0, 0, d, c]
            k2 = k1 + doffs[0, 0, d, c]
            w1 = dwts[0, 0, 0, d, c]
            w2 = dwts[1, 0, 0, d, c]
            p1 = lax.div(k1, points)
            n1 = lax.rem(k1, points) + PAD
            p2 = lax.div(k2, points)
            n2 = lax.rem(k2, points) + PAD
            for v in range(nv):
                dsend[d, v, pl.ds(c, 1), :] = w1 * ext[v, p1, pl.ds(n1, 1), :] + w2 * ext[v, p2, pl.ds(n2, 1), :]
            return carry

        lax.fori_loop(0, cap, one, 0, unroll=4)

    def donor_copy(d):
        return pltpu.make_async_remote_copy(
            src_ref=dsend.at[d], dst_ref=drecv.at[me], send_sem=dsend_s.at[d], recv_sem=drecv_s.at[me],
            device_id=(d, l), device_id_type=MESH)

    for d in peers:
        gather(d)
        donor_copy(d).start()
    gather(me)
    local_copy = pltpu.make_async_copy(dsend.at[me], drecv.at[me], dloc_s.at[0])
    local_copy.start()

    lane = lax.broadcasted_iota(jnp.int32, (points, width), 1)
    row = lax.broadcasted_iota(jnp.int32, (points, width), 0)
    lane1 = lax.broadcasted_iota(jnp.int32, (1, width), 1)
    mix = []
    for v in range(nv):
        m = jnp.zeros((1, width), F32)
        for u in range(nv):
            m = jnp.where(lane1 // 4 == u, -right_eig[v, u], m)
        mix.append(m)

    zero_pad = jnp.zeros((PAD, width), F32)
    lower_in.wait()
    upper_in.wait()

    def spread(block, r, c):
        return jnp.broadcast_to(block[r:r + 1, c:c + 1], (1, width))

    last = points - 1

    def prepare(p, carry):
        at = pl.ds(p, 1)
        packed = jnp.zeros((points, width), F32)
        for v in range(nv):
            ext[v, p, 0:PAD, :] = zero_pad
            ext[v, p, PAD + points:PAD + points + PAD, :] = zero_pad
            lo_block = lbuf[v, p]
            up_block = ubuf[v, p]
            h, o = split(lo_block)
            lsp[v, p, :, 0:points] = h
            lsp[v, p, :, points:2 * points] = o
            h, o = split(up_block)
            usp[v, p, :, 0:points] = h
            usp[v, p, :, points:2 * points] = o
            acor[0, 0, v, at, :] = spread(lo_block, last, 0)
            acor[0, 1, v, at, :] = spread(lo_block, last, 1)
            acor[0, 2, v, at, :] = spread(lo_block, last - 1, 0)
            acor[0, 3, v, at, :] = spread(lo_block, last - 1, 1)
            acor[1, 0, v, at, :] = spread(up_block, 0, last)
            acor[1, 1, v, at, :] = spread(up_block, 0, last - 1)
            acor[1, 2, v, at, :] = spread(up_block, 1, last)
            acor[1, 3, v, at, :] = spread(up_block, 1, last - 1)
            rolled = pltpu.roll(lo_block, 4 * v, 1) if v else lo_block
            unit = ((lane == 4 * v + 2) & (row == last)) | ((lane == 4 * v + 3) & (row == last - 1))
            cols = jnp.where((lane == 4 * v) | (lane == 4 * v + 1), rolled, jnp.where(unit, 1.0, 0.0))
            packed = packed + product(jnp.concatenate([h, o], axis=1), cols)
        for v in range(nv):
            for j in range(2):
                for k in range(2):
                    cor[j, k, v, at, :] = spread(packed, j, 4 * v + k)
            scaled = packed * mix[v]
            h, o = split(scaled)
            hf = h.astype(F32)
            stacked = hf + pltpu.roll(o.astype(F32), 32, 1) + pltpu.roll(hf, 64, 1)
            lhs[p, v * points:(v + 1) * points, :] = stacked.astype(BF16)
        return carry

    lax.fori_loop(0, planes, prepare, 0)

    for side, link in ((0, llink), (1, ulink)):
        for v in range(nv):
            c0, c1, c2 = link[0, v], link[1, v], link[2, v]
            a00, a01, a10, a11 = (acor[side, i, v] for i in range(4))
            amine[side, 0, v] = -(a00 * c0 + a01 * c2)
            amine[side, 1, v] = -a00 * c1
            amine[side, 2, v] = -(a10 * c0 + a11 * c2)
            amine[side, 3, v] = -a10 * c1

    def swap_copy(src, dst, send, recv):
        return pltpu.make_async_remote_copy(src_ref=src, dst_ref=dst, send_sem=send, recv_sem=recv,
                                            device_id=(me, partner), device_id_type=MESH)

    map_copies = [swap_copy(amine.at[s], atheirs.at[s], asend_s.at[s], arecv_s.at[s]) for s in range(2)]
    for copy in map_copies:
        copy.start()

    for d in peers:
        pltpu.make_async_remote_copy(
            src_ref=dsend.at[d], dst_ref=drecv.at[d], send_sem=dsend_s.at[d], recv_sem=drecv_s.at[d],
            device_id=(d, l), device_id_type=MESH).wait_recv()
    local_copy.wait()
    slots = np_ * cap
    for s in range(np_):
        for v in range(nv):
            h, o = split(drecv[s, v])
            rhs[s * cap:(s + 1) * cap, v * width:(v + 1) * width] = h
            rhs[slots + s * cap:slots + (s + 1) * cap, v * width:(v + 1) * width] = o
    rhs[0:slots, nv * width:(nv + 1) * width] = jnp.ones((slots, width), BF16)
    rhs[slots:2 * slots, nv * width:(nv + 1) * width] = jnp.zeros((slots, width), BF16)
    slot_lane = lax.broadcasted_iota(jnp.int32, (1, cap), 1)
    targets = jnp.concatenate(
        [jnp.where(slot_lane < counts[s, 0, 0], rrows[0, 0, s:s + 1, :], planes * points) for s in range(np_)], axis=1)
    target_all = jnp.broadcast_to(targets, (points, slots))
    row_slot = lax.broadcasted_iota(jnp.int32, (points, slots), 0)
    wave_in.wait()

    def scatter(p, carry):
        hot = jnp.where(target_all == row_slot + p * points, 1.0, 0.0).astype(BF16)
        hot2 = jnp.concatenate([hot, hot], axis=1)
        vals = jnp.dot(hot2, rhs[...], preferred_element_type=F32)
        taken = vals[:, nv * width:] > 0.5
        at = pl.ds(p, 1)
        for v in range(nv):
            new = jnp.where(taken, vals[:, v * width:(v + 1) * width], ext[v, p, PAD:PAD + points, :])
            ext[v, p, PAD:PAD + points, :] = new
            for j in range(2):
                hsend[0, j, v, at, :] = new[j:j + 1]
                hsend[1, j, v, at, :] = new[last - j:last - j + 1]
        wedge[0, at, :] = wbuf[p, 0:1, :]
        wedge[1, at, :] = wbuf[p, 1:2, :]
        wedge[2, at, :] = wbuf[p, last:last + 1, :]
        wedge[3, at, :] = wbuf[p, last - 1:last, :]
        return carry

    lax.fori_loop(0, planes, scatter, 0)

    down_copy = pltpu.make_async_remote_copy(src_ref=hsend.at[0], dst_ref=hrecv.at[1], send_sem=hsend_s.at[0],
                                             recv_sem=hrecv_s.at[1], device_id=(me, l - 1), device_id_type=MESH)
    up_copy = pltpu.make_async_remote_copy(src_ref=hsend.at[1], dst_ref=hrecv.at[0], send_sem=hsend_s.at[1],
                                           recv_sem=hrecv_s.at[0], device_id=(me, l + 1), device_id_type=MESH)

    @pl.when(l > 0)
    def _():
        down_copy.start()

    @pl.when(l < nl_ - 1)
    def _():
        up_copy.start()

    @pl.when(l == 0)
    def _():
        hrecv[0] = jnp.zeros(hrecv.shape[1:], F32)

    @pl.when(l == nl_ - 1)
    def _():
        hrecv[1] = jnp.zeros(hrecv.shape[1:], F32)

    piece = 32
    lane_p = lax.broadcasted_iota(jnp.int32, (piece, width), 1)
    first_lane = lane_p == 0
    final_lane = lane_p == width - 1

    def derive(p, carry):
        for part in range(points // piece):
            base = part * piece
            ws = -wbuf[p, base:base + piece, :]
            tends = []
            for u in range(nv):
                o = PAD + base
                mid = ext[u, p, o:o + piece, :]
                n1 = ext[u, p, o + 1:o + 1 + piece, :]
                n2 = ext[u, p, o + 2:o + 2 + piece, :]
                b1 = ext[u, p, o - 1:o - 1 + piece, :]
                b2 = ext[u, p, o - 2:o - 2 + piece, :]
                right = jnp.where(final_lane, 0.0, pltpu.roll(mid, width - 1, 1))
                left = jnp.where(first_lane, 0.0, pltpu.roll(mid, 1, 1))
                total = 0.5 * (right - left) + 0.25 * n1 - 0.75 * b1 + 0.375 * mid + 0.0625 * (n2 + b2)
                tends.append(ws * total)
            for v in range(nv):
                acc = left_eig[v, 0] * tends[0]
                for u in range(1, nv):
                    acc = acc + left_eig[v, u] * tends[u]
                char[v, p, base:base + piece, :] = acc
        return carry

    lax.fori_loop(0, planes, derive, 0)

    @pl.when(l > 0)
    def _():
        up_copy.wait_recv()

    @pl.when(l < nl_ - 1)
    def _():
        down_copy.wait_recv()

    tb1 = [hrecv[0, 0, u] for u in range(nv)]
    tb2 = [hrecv[0, 1, u] for u in range(nv)]
    ta1 = [hrecv[1, 0, u] for u in range(nv)]
    ta2 = [hrecv[1, 1, u] for u in range(nv)]
    for v in range(nv):
        acc = [jnp.zeros((planes, width), F32) for _ in range(4)]
        for u in range(nv):
            e = left_eig[v, u]
            acc[0] = acc[0] + e * (-0.75 * tb1[u] + 0.0625 * tb2[u])
            acc[1] = acc[1] + e * (0.0625 * tb1[u])
            acc[2] = acc[2] + e * (0.25 * ta1[u] + 0.0625 * ta2[u])
            acc[3] = acc[3] + e * (0.0625 * ta1[u])
        for j in range(4):
            cfix[j, v] = -wedge[j] * acc[j]

    def lower_pass(p, carry):
        chunk = p // SUB
        at = pl.ds(p % SUB, 1)
        here = pl.ds(p, 1)
        for v in range(nv):
            for j, r in enumerate((0, 1, last, last - 1)):
                char[v, p, r:r + 1, :] = char[v, p, r:r + 1, :] + cfix[j, v, here, :]
            y = product(lsp[v, p], char[v, p])
            char[v, p] = y
            bmine[0, chunk, 0, v, at, :] = y[last:last + 1]
            bmine[0, chunk, 1, v, at, :] = y[last - 1:last]
        return carry

    def b_copy(side, c):
        return swap_copy(bmine.at[side, c], btheirs.at[side, c], bsend_s.at[side, c], brecv_s.at[side, c])

    for c in range(chunks):
        lax.fori_loop(c * SUB, (c + 1) * SUB, lower_pass, 0)
        b_copy(0, c).start()

    for copy in map_copies:
        copy.wait_recv()

    def chain_copy(side, c):
        to = l + 2 if side == 0 else l - 2
        return pltpu.make_async_remote_copy(
            src_ref=fsend.at[side, c], dst_ref=fin.at[side, c], send_sem=csend_s.at[side, c],
            recv_sem=crecv_s.at[side, c], device_id=(me, to), device_id_type=MESH)

    def has_before(side):
        return z > 0 if side == 0 else z < nz - 1

    def has_after(side):
        return z < nz - 1 if side == 0 else z > 0

    def relay(side, c):
        b_copy(side, c).wait_recv()
        second = x == 1 if side == 0 else x == 0

        @pl.when(has_before(side))
        def _():
            chain_copy(side, c).wait_recv()

        @pl.when(jnp.logical_not(has_before(side)))
        def _():
            fin[side, c] = jnp.zeros(fin.shape[2:], F32)

        sl = slice(c * SUB, (c + 1) * SUB)
        for v in range(nv):
            y1, y2 = fin[side, c, 0, v], fin[side, c, 1, v]
            am = [amine[side, i, v, sl] for i in range(4)]
            at_ = [atheirs[side, i, v, sl] for i in range(4)]
            bm = [bmine[side, c, i, v] for i in range(2)]
            bt = [btheirs[side, c, i, v] for i in range(2)]
            a1 = [jnp.where(second, t, m) for m, t in zip(am, at_)]
            a2 = [jnp.where(second, m, t) for m, t in zip(am, at_)]
            b1 = [jnp.where(second, t, m) for m, t in zip(bm, bt)]
            b2 = [jnp.where(second, m, t) for m, t in zip(bm, bt)]
            m1 = a1[0] * y1 + a1[1] * y2 + b1[0]
            m2 = a1[2] * y1 + a1[3] * y2 + b1[1]
            fsend[side, c, 0, v] = a2[0] * m1 + a2[1] * m2 + b2[0]
            fsend[side, c, 1, v] = a2[2] * m1 + a2[3] * m2 + b2[1]
            fin[side, c, 0, v] = jnp.where(second, m1, y1)
            fin[side, c, 1, v] = jnp.where(second, m2, y2)

        @pl.when(has_after(side))
        def _():
            chain_copy(side, c).start()

    def upper_pass(p, carry):
        here = pl.ds(p, 1)
        for v in range(nv):
            y = product(usp[v, p], char[v, p])
            char[v, p] = y
            ubrow[0, v, here, :] = y[0:1]
            ubrow[1, v, here, :] = y[1:2]
        for part in range(points // piece):
            base = part * piece
            ups = [char[u, p, base:base + piece, :] for u in range(nv)]
            for v in range(nv):
                acc = ext[v, p, PAD + base:PAD + base + piece, :]
                for u in range(nv):
                    acc = acc + right_eig[v, u] * ups[u]
                obuf[v, p, base:base + piece, :] = acc
        return carry

    def back_offset(c):
        sl = slice(c * SUB, (c + 1) * SUB)
        for v in range(nv):
            y1, y2 = fin[0, c, 0, v], fin[0, c, 1, v]
            f = llink[0, v, sl] * y1 + llink[1, v, sl] * y2
            s = llink[2, v, sl] * y1
            rows[c, 4 * v] = f
            rows[c, 4 * v + 1] = s
            for j in range(2):
                bmine[1, c, j, v] = ubrow[j, v, sl] - cor[j, 0, v, sl] * f - cor[j, 1, v, sl] * s
        b_copy(1, c).start()

    for c in range(chunks):
        lax.fori_loop(c * SUB, (c + 1) * SUB, upper_pass, 0)
        relay(0, c)
        back_offset(c)

    nk = 4 * nv
    out_copies = []
    for c in range(chunks):
        relay(1, c)
        sl = slice(c * SUB, (c + 1) * SUB)
        for v in range(nv):
            x1, x2 = fin[1, c, 0, v], fin[1, c, 1, v]
            rows[c, 4 * v + 2] = ulink[0, v, sl] * x1 + ulink[1, v, sl] * x2
            rows[c, 4 * v + 3] = ulink[2, v, sl] * x1

        def finish(q, carry):
            p = c * SUB + q
            r = jnp.concatenate([rows[c, k, pl.ds(q, 1), :] for k in range(nk)]
                                + [jnp.zeros((32 - nk, width), F32)], axis=0)
            h = r.astype(BF16).astype(F32)
            o = r - h
            right = jnp.concatenate([h, h, o, jnp.zeros((width - 96, width), F32)], axis=0).astype(BF16)
            for v in range(nv):
                add = jnp.dot(lhs[p, v * points:(v + 1) * points, :], right, preferred_element_type=F32)
                obuf[v, p] = obuf[v, p] + add
            return carry

        lax.fori_loop(0, SUB, finish, 0)
        copy = pltpu.make_async_copy(obuf.at[:, pl.ds(c * SUB, SUB)], out.at[:, pl.ds(c * SUB, SUB)], osem.at[c])
        copy.start()
        out_copies.append(copy)

    for d in peers:
        donor_copy(d).wait_send()
    for copy in map_copies:
        copy.wait_send()

    @pl.when(l > 0)
    def _():
        down_copy.wait_send()

    @pl.when(l < nl_ - 1)
    def _():
        up_copy.wait_send()

    for side in range(2):
        for c in range(chunks):
            b_copy(side, c).wait_send()

            @pl.when(has_after(side))
            def _():
                chain_copy(side, c).wait_send()
    for copy in out_copies:
        copy.wait()


def local(np_, nl_, flow_state, wave_speed, left_eig, right_eig, lower_inverse, upper_inverse, lower_link, upper_link,
          donor_rows, stencil_offsets, donor_weights, block_counts, receptor_rows):
    nv, planes, points, width = flow_state.shape
    chunks = planes // SUB
    cap = donor_rows.shape[3]
    slots = np_ * cap
    vmem = pl.BlockSpec(memory_space=pltpu.VMEM)
    smem = pl.BlockSpec(memory_space=pltpu.SMEM)
    hbm = pl.BlockSpec(memory_space=pl.ANY)
    dma = pltpu.SemaphoreType.DMA
    state = (2, chunks, 2, nv, SUB, width)
    return pl.pallas_call(
        functools.partial(kernel, np_, nl_),
        out_shape=jax.ShapeDtypeStruct(flow_state.shape, F32),
        in_specs=[hbm, hbm, hbm, hbm, smem, smem, vmem, vmem, smem, smem, smem, smem, vmem],
        out_specs=hbm,
        scratch_shapes=[
            pltpu.VMEM((nv, planes, points + 2 * PAD, width), F32),
            pltpu.VMEM((planes, points, width), F32),
            pltpu.VMEM((nv, planes, points, points), F32),
            pltpu.VMEM((nv, planes, points, points), F32),
            pltpu.VMEM((nv, planes, points, 2 * points), BF16),
            pltpu.VMEM((nv, planes, points, 2 * points), BF16),
            pltpu.VMEM((nv, planes, points, width), F32),
            pltpu.VMEM((nv, planes, points, width), F32),
            pltpu.VMEM((planes, nv * points, width), BF16),
            pltpu.VMEM((np_, nv, cap, width), F32),
            pltpu.VMEM((np_, nv, cap, width), F32),
            pltpu.VMEM((2 * slots, (nv + 1) * width), BF16),
            pltpu.VMEM((2, 2, nv, planes, width), F32),
            pltpu.VMEM((2, 2, nv, planes, width), F32),
            pltpu.VMEM((4, planes, width), F32),
            pltpu.VMEM((4, nv, planes, width), F32),
            pltpu.VMEM((2, 4, nv, planes, width), F32),
            pltpu.VMEM((2, 4, nv, planes, width), F32),
            pltpu.VMEM(state, F32),
            pltpu.VMEM(state, F32),
            pltpu.VMEM(state, F32),
            pltpu.VMEM(state, F32),
            pltpu.VMEM((2, nv, planes, width), F32),
            pltpu.VMEM((2, 2, nv, planes, width), F32),
            pltpu.VMEM((2, 4, nv, planes, width), F32),
            pltpu.VMEM((chunks, 4 * nv, SUB, width), F32),
            dma((4,)), dma((chunks,)), dma((np_,)), dma((np_,)), dma((1,)), dma((2,)), dma((2,)), dma((2,)), dma((2,)),
            dma((2, chunks)), dma((2, chunks)), dma((2, chunks)), dma((2, chunks)),
        ],
        compiler_params=pltpu.CompilerParams(
            collective_id=0, has_side_effects=True, vmem_limit_bytes=60 * 1024 * 1024),
    )(flow_state, wave_speed, lower_inverse, upper_inverse, left_eig, right_eig,
      lower_link.reshape(lower_link.shape[:3] + (width,)), upper_link.reshape(upper_link.shape[:3] + (width,)),
      donor_rows, stencil_offsets, donor_weights, block_counts, receptor_rows)


def solution(mesh):
    in_specs = (
        P(None, "plane", "line", None),
        P("plane", "line", None),
        P(),
        P(),
        P(None, "plane", "line", None),
        P(None, "plane", "line", None),
        P(None, None, "plane", "line", None),
        P(None, None, "plane", "line", None),
        P("plane", "line", None, None),
        P("plane", "line", None, None),
        P(None, "plane", "line", None, None),
        P(None, "line", "plane"),
        P("plane", "line", None, None),
    )
    out_specs = P(None, "plane", "line", None)
    body = functools.partial(local, mesh.shape["plane"], mesh.shape["line"])
    return jax.shard_map(body, mesh=mesh, in_specs=in_specs, out_specs=out_specs, check_vma=False)
```

```python
import functools
import jax
import jax.numpy as jnp
from jax import lax
from jax.experimental import pallas as pl
from jax.experimental.pallas import tpu as pltpu
from jax.sharding import PartitionSpec as P

MESH = pl.DeviceIdType.MESH
F32 = jnp.float32
BF16 = jnp.bfloat16
PAD = 8
SUB = 8


def split(x):
    hi = x.astype(BF16)
    lo = (x - hi.astype(F32)).astype(BF16)
    return hi, lo


def wide(x):
    hi, lo = split(x)
    both = jnp.concatenate([hi, lo], axis=1)
    return jnp.concatenate([both, both], axis=0)


def product(left_pair, x):
    n = x.shape[1]
    full = jnp.dot(left_pair, wide(x), preferred_element_type=F32)
    return full[:, :n] + full[:, n:]


def kernel(
    np_, nl_, flow, wave, lower, upper, left_eig, right_eig, llink, ulink, drows, doffs, dwts, counts, rrows,
    obuf,
    ext, wbuf, lbuf, ubuf, lsp, usp, char, packs, lhs, dsend, drecv, rhs, hsend, hrecv, wedge, cfix,
    amine, atheirs, bmine, btheirs, fin, fsend, ubrow, cor, acor, rows,
    lsem, dsend_s, drecv_s, dloc_s, hsend_s, hrecv_s, asend_s, arecv_s, bsend_s, brecv_s, csend_s, crecv_s,
):
    nv, planes, points, width = lower.shape
    chunks = planes // SUB
    cap = drows.shape[3]
    me = lax.axis_index("plane")
    l = lax.axis_index("line")
    z = l // 2
    x = l % 2
    nz = nl_ // 2
    partner = l + 1 - 2 * x

    barrier = pltpu.get_barrier_semaphore()
    own_chip = me // 2
    peers = [((own_chip + 1 + i) % (np_ // 2)) * 2 + c for i in range(np_ // 2 - 1) for c in (0, 1)]
    peers.append(own_chip * 2 + 1 - me % 2)
    for d in peers:
        pl.semaphore_signal(barrier, inc=1, device_id=(d, l), device_id_type=MESH)
    for step in (1, 2):
        @pl.when(l >= step)
        def _():
            pl.semaphore_signal(barrier, inc=1, device_id=(me, l - step), device_id_type=MESH)

        @pl.when(l + step < nl_)
        def _():
            pl.semaphore_signal(barrier, inc=1, device_id=(me, l + step), device_id_type=MESH)

    flow_in = pltpu.make_async_copy(flow, ext.at[:, :, pl.ds(PAD, points), :], lsem.at[0])
    lower_in = pltpu.make_async_copy(lower, lbuf, lsem.at[1])
    upper_in = pltpu.make_async_copy(upper, ubuf, lsem.at[2])
    wave_in = pltpu.make_async_copy(wave, wbuf, lsem.at[3])
    flow_in.start()
    lower_in.start()
    upper_in.start()
    wave_in.start()

    near = jnp.minimum(l, 2) + jnp.minimum(nl_ - 1 - l, 2)
    pl.semaphore_wait(barrier, len(peers) + near)

    flow_in.wait()

    def gather(d):
        def one(c, carry):
            k1 = drows[0, 0, d, c]
            k2 = k1 + doffs[0, 0, d, c]
            w1 = dwts[0, 0, 0, d, c]
            w2 = dwts[1, 0, 0, d, c]
            p1 = lax.div(k1, points)
            n1 = lax.rem(k1, points) + PAD
            p2 = lax.div(k2, points)
            n2 = lax.rem(k2, points) + PAD
            for v in range(nv):
                dsend[d, v, pl.ds(c, 1), :] = w1 * ext[v, p1, pl.ds(n1, 1), :] + w2 * ext[v, p2, pl.ds(n2, 1), :]
            return carry

        lax.fori_loop(0, cap, one, 0, unroll=4)

    def donor_copy(d):
        return pltpu.make_async_remote_copy(
            src_ref=dsend.at[d], dst_ref=drecv.at[me], send_sem=dsend_s.at[d], recv_sem=drecv_s.at[me],
            device_id=(d, l), device_id_type=MESH)

    for d in peers:
        gather(d)
        donor_copy(d).start()
    gather(me)
    local_copy = pltpu.make_async_copy(dsend.at[me], drecv.at[me], dloc_s.at[0])
    local_copy.start()

    lane = lax.broadcasted_iota(jnp.int32, (points, width), 1)
    row = lax.broadcasted_iota(jnp.int32, (points, width), 0)
    lane1 = lax.broadcasted_iota(jnp.int32, (1, width), 1)
    mix = []
    for v in range(nv):
        m = jnp.zeros((1, width), F32)
        for u in range(nv):
            m = jnp.where(lane1 // 4 == u, -right_eig[v, u], m)
        mix.append(m)

    zero_pad = jnp.zeros((PAD, width), F32)
    lower_in.wait()
    upper_in.wait()

    def spread(block, r, c):
        return jnp.broadcast_to(block[r:r + 1, c:c + 1], (1, width))

    last = points - 1

    def prepare(p, carry):
        at = pl.ds(p, 1)
        for v in range(nv):
            ext[v, p, 0:PAD, :] = zero_pad
            ext[v, p, PAD + points:PAD + points + PAD, :] = zero_pad
            lo_block = lbuf[v, p]
            up_block = ubuf[v, p]
            h, o = split(lo_block)
            lsp[v, p, :, 0:points] = h
            lsp[v, p, :, points:2 * points] = o
            h, o = split(up_block)
            usp[v, p, :, 0:points] = h
            usp[v, p, :, points:2 * points] = o
            acor[0, 0, v, at, :] = spread(lo_block, last, 0)
            acor[0, 1, v, at, :] = spread(lo_block, last, 1)
            acor[0, 2, v, at, :] = spread(lo_block, last - 1, 0)
            acor[0, 3, v, at, :] = spread(lo_block, last - 1, 1)
            acor[1, 0, v, at, :] = spread(up_block, 0, last)
            acor[1, 1, v, at, :] = spread(up_block, 0, last - 1)
            acor[1, 2, v, at, :] = spread(up_block, 1, last)
            acor[1, 3, v, at, :] = spread(up_block, 1, last - 1)
        return carry

    lax.fori_loop(0, planes, prepare, 0)

    for side, link in ((0, llink), (1, ulink)):
        for v in range(nv):
            c0, c1, c2 = link[0, v], link[1, v], link[2, v]
            a00, a01, a10, a11 = (acor[side, i, v] for i in range(4))
            amine[side, 0, v] = -(a00 * c0 + a01 * c2)
            amine[side, 1, v] = -a00 * c1
            amine[side, 2, v] = -(a10 * c0 + a11 * c2)
            amine[side, 3, v] = -a10 * c1

    def swap_copy(src, dst, send, recv):
        return pltpu.make_async_remote_copy(src_ref=src, dst_ref=dst, send_sem=send, recv_sem=recv,
                                            device_id=(me, partner), device_id_type=MESH)

    map_copies = [swap_copy(amine.at[s], atheirs.at[s], asend_s.at[s], arecv_s.at[s]) for s in range(2)]
    for copy in map_copies:
        copy.start()

    for d in peers:
        pltpu.make_async_remote_copy(
            src_ref=dsend.at[d], dst_ref=drecv.at[d], send_sem=dsend_s.at[d], recv_sem=drecv_s.at[d],
            device_id=(d, l), device_id_type=MESH).wait_recv()
    local_copy.wait()
    slots = np_ * cap
    for s in range(np_):
        for v in range(nv):
            h, o = split(drecv[s, v])
            rhs[s * cap:(s + 1) * cap, v * width:(v + 1) * width] = h
            rhs[slots + s * cap:slots + (s + 1) * cap, v * width:(v + 1) * width] = o
    rhs[0:slots, nv * width:(nv + 1) * width] = jnp.ones((slots, width), BF16)
    rhs[slots:2 * slots, nv * width:(nv + 1) * width] = jnp.zeros((slots, width), BF16)
    slot_lane = lax.broadcasted_iota(jnp.int32, (1, cap), 1)
    targets = jnp.concatenate(
        [jnp.where(slot_lane < counts[0, 0, s], rrows[0, 0, s:s + 1, :], planes * points) for s in range(np_)], axis=1)
    target_all = jnp.broadcast_to(targets, (points, slots))
    row_slot = lax.broadcasted_iota(jnp.int32, (points, slots), 0)
    wave_in.wait()

    def scatter(p, carry):
        hot = jnp.where(target_all == row_slot + p * points, 1.0, 0.0).astype(BF16)
        hot2 = jnp.concatenate([hot, hot], axis=1)
        vals = jnp.dot(hot2, rhs[...], preferred_element_type=F32)
        taken = vals[:, nv * width:] > 0.5
        at = pl.ds(p, 1)
        for v in range(nv):
            new = jnp.where(taken, vals[:, v * width:(v + 1) * width], ext[v, p, PAD:PAD + points, :])
            ext[v, p, PAD:PAD + points, :] = new
            for j in range(2):
                hsend[0, j, v, at, :] = new[j:j + 1]
                hsend[1, j, v, at, :] = new[last - j:last - j + 1]
        wedge[0, at, :] = wbuf[p, 0:1, :]
        wedge[1, at, :] = wbuf[p, 1:2, :]
        wedge[2, at, :] = wbuf[p, last:last + 1, :]
        wedge[3, at, :] = wbuf[p, last - 1:last, :]
        return carry

    lax.fori_loop(0, planes, scatter, 0)

    down_copy = pltpu.make_async_remote_copy(src_ref=hsend.at[0], dst_ref=hrecv.at[1], send_sem=hsend_s.at[0],
                                             recv_sem=hrecv_s.at[1], device_id=(me, l - 1), device_id_type=MESH)
    up_copy = pltpu.make_async_remote_copy(src_ref=hsend.at[1], dst_ref=hrecv.at[0], send_sem=hsend_s.at[1],
                                           recv_sem=hrecv_s.at[0], device_id=(me, l + 1), device_id_type=MESH)

    @pl.when(l > 0)
    def _():
        down_copy.start()

    @pl.when(l < nl_ - 1)
    def _():
        up_copy.start()

    @pl.when(l == 0)
    def _():
        hrecv[0] = jnp.zeros(hrecv.shape[1:], F32)

    @pl.when(l == nl_ - 1)
    def _():
        hrecv[1] = jnp.zeros(hrecv.shape[1:], F32)

    piece = 32
    lane_p = lax.broadcasted_iota(jnp.int32, (piece, width), 1)
    first_lane = lane_p == 0
    final_lane = lane_p == width - 1

    def derive(p, carry):
        for part in range(points // piece):
            base = part * piece
            ws = -wbuf[p, base:base + piece, :]
            tends = []
            for u in range(nv):
                o = PAD + base
                mid = ext[u, p, o:o + piece, :]
                n1 = ext[u, p, o + 1:o + 1 + piece, :]
                n2 = ext[u, p, o + 2:o + 2 + piece, :]
                b1 = ext[u, p, o - 1:o - 1 + piece, :]
                b2 = ext[u, p, o - 2:o - 2 + piece, :]
                right = jnp.where(final_lane, 0.0, pltpu.roll(mid, width - 1, 1))
                left = jnp.where(first_lane, 0.0, pltpu.roll(mid, 1, 1))
                total = 0.5 * (right - left) + 0.25 * n1 - 0.75 * b1 + 0.375 * mid + 0.0625 * (n2 + b2)
                tends.append(ws * total)
            for v in range(nv):
                acc = left_eig[v, 0] * tends[0]
                for u in range(1, nv):
                    acc = acc + left_eig[v, u] * tends[u]
                char[v, p, base:base + piece, :] = acc
        return carry

    lax.fori_loop(0, planes, derive, 0)

    @pl.when(l > 0)
    def _():
        up_copy.wait_recv()

    @pl.when(l < nl_ - 1)
    def _():
        down_copy.wait_recv()

    tb1 = [hrecv[0, 0, u] for u in range(nv)]
    tb2 = [hrecv[0, 1, u] for u in range(nv)]
    ta1 = [hrecv[1, 0, u] for u in range(nv)]
    ta2 = [hrecv[1, 1, u] for u in range(nv)]
    for v in range(nv):
        acc = [jnp.zeros((planes, width), F32) for _ in range(4)]
        for u in range(nv):
            e = left_eig[v, u]
            acc[0] = acc[0] + e * (-0.75 * tb1[u] + 0.0625 * tb2[u])
            acc[1] = acc[1] + e * (0.0625 * tb1[u])
            acc[2] = acc[2] + e * (0.25 * ta1[u] + 0.0625 * ta2[u])
            acc[3] = acc[3] + e * (0.0625 * ta1[u])
        for j in range(4):
            cfix[j, v] = -wedge[j] * acc[j]

    def pack(p, carry):
        at = pl.ds(p, 1)
        packed = jnp.zeros((points, width), F32)
        for v in range(nv):
            lo_block = lbuf[v, p]
            rolled = pltpu.roll(lo_block, 4 * v, 1) if v else lo_block
            unit = ((lane == 4 * v + 2) & (row == last)) | ((lane == 4 * v + 3) & (row == last - 1))
            cols = jnp.where((lane == 4 * v) | (lane == 4 * v + 1), rolled, jnp.where(unit, 1.0, 0.0))
            packed = packed + product(usp[v, p], cols)
        for v in range(nv):
            for j in range(2):
                for k in range(2):
                    cor[j, k, v, at, :] = spread(packed, j, 4 * v + k)
        packs[p] = packed
        return carry

    def scale(p, carry):
        packed = packs[p]
        for v in range(nv):
            scaled = packed * mix[v]
            h, o = split(scaled)
            hf = h.astype(F32)
            stacked = hf + pltpu.roll(o.astype(F32), 32, 1) + pltpu.roll(hf, 64, 1)
            lhs[p, v * points:(v + 1) * points, :] = stacked.astype(BF16)
        return carry

    def lower_pass(p, carry):
        chunk = p // SUB
        at = pl.ds(p % SUB, 1)
        here = pl.ds(p, 1)
        for v in range(nv):
            for j, r in enumerate((0, 1, last, last - 1)):
                char[v, p, r:r + 1, :] = char[v, p, r:r + 1, :] + cfix[j, v, here, :]
            y = product(lsp[v, p], char[v, p])
            char[v, p] = y
            bmine[0, chunk, 0, v, at, :] = y[last:last + 1]
            bmine[0, chunk, 1, v, at, :] = y[last - 1:last]
        return carry

    def b_copy(side, c):
        return swap_copy(bmine.at[side, c], btheirs.at[side, c], bsend_s.at[side, c], brecv_s.at[side, c])

    for c in range(chunks):
        lax.fori_loop(c * SUB, (c + 1) * SUB, lower_pass, 0)
        b_copy(0, c).start()

    for copy in map_copies:
        copy.wait_recv()

    def chain_copy(side, c):
        to = l + 2 if side == 0 else l - 2
        return pltpu.make_async_remote_copy(
            src_ref=fsend.at[side, c], dst_ref=fin.at[side, c], send_sem=csend_s.at[side, c],
            recv_sem=crecv_s.at[side, c], device_id=(me, to), device_id_type=MESH)

    def has_before(side):
        return z > 0 if side == 0 else z < nz - 1

    def has_after(side):
        return z < nz - 1 if side == 0 else z > 0

    def relay(side, c):
        b_copy(side, c).wait_recv()
        second = x == 1 if side == 0 else x == 0

        @pl.when(has_before(side))
        def _():
            chain_copy(side, c).wait_recv()

        @pl.when(jnp.logical_not(has_before(side)))
        def _():
            fin[side, c] = jnp.zeros(fin.shape[2:], F32)

        sl = slice(c * SUB, (c + 1) * SUB)
        for v in range(nv):
            y1, y2 = fin[side, c, 0, v], fin[side, c, 1, v]
            am = [amine[side, i, v, sl] for i in range(4)]
            at_ = [atheirs[side, i, v, sl] for i in range(4)]
            bm = [bmine[side, c, i, v] for i in range(2)]
            bt = [btheirs[side, c, i, v] for i in range(2)]
            a1 = [jnp.where(second, t, m) for m, t in zip(am, at_)]
            a2 = [jnp.where(second, m, t) for m, t in zip(am, at_)]
            b1 = [jnp.where(second, t, m) for m, t in zip(bm, bt)]
            b2 = [jnp.where(second, m, t) for m, t in zip(bm, bt)]
            m1 = a1[0] * y1 + a1[1] * y2 + b1[0]
            m2 = a1[2] * y1 + a1[3] * y2 + b1[1]
            fsend[side, c, 0, v] = a2[0] * m1 + a2[1] * m2 + b2[0]
            fsend[side, c, 1, v] = a2[2] * m1 + a2[3] * m2 + b2[1]
            fin[side, c, 0, v] = jnp.where(second, m1, y1)
            fin[side, c, 1, v] = jnp.where(second, m2, y2)

        @pl.when(has_after(side))
        def _():
            chain_copy(side, c).start()

    def upper_pass(p, carry):
        here = pl.ds(p, 1)
        for v in range(nv):
            y = product(usp[v, p], char[v, p])
            char[v, p] = y
            ubrow[0, v, here, :] = y[0:1]
            ubrow[1, v, here, :] = y[1:2]
        for part in range(points // piece):
            base = part * piece
            ups = [char[u, p, base:base + piece, :] for u in range(nv)]
            for v in range(nv):
                acc = ext[v, p, PAD + base:PAD + base + piece, :]
                for u in range(nv):
                    acc = acc + right_eig[v, u] * ups[u]
                obuf[v, p, base:base + piece, :] = acc
        return carry

    def back_offset(c):
        sl = slice(c * SUB, (c + 1) * SUB)
        for v in range(nv):
            y1, y2 = fin[0, c, 0, v], fin[0, c, 1, v]
            f = llink[0, v, sl] * y1 + llink[1, v, sl] * y2
            s = llink[2, v, sl] * y1
            rows[c, 4 * v] = f
            rows[c, 4 * v + 1] = s
            for j in range(2):
                bmine[1, c, j, v] = ubrow[j, v, sl] - cor[j, 0, v, sl] * f - cor[j, 1, v, sl] * s
        b_copy(1, c).start()

    def work(body, c):
        lax.fori_loop(c * SUB, (c + 1) * SUB, body, 0)

    slots_of = [(pack, c) for c in range(chunks)] + [(upper_pass, c) for c in range(chunks)]
    for turn in range(len(slots_of) + chunks):
        for c in range(chunks):
            spot = turn - c
            if 0 <= spot < len(slots_of):
                @pl.when(z == spot if spot < len(slots_of) - 1 else z >= spot)
                def _():
                    relay(0, c)
                if spot == len(slots_of) - 1:
                    back_offset(c)
        if turn < len(slots_of):
            work(*slots_of[turn])

    @pl.when(z == nz - 1)
    def _():
        for c in range(chunks):
            relay(1, c)

    lax.fori_loop(0, planes, scale, 0)

    @pl.when(z < nz - 1)
    def _():
        for c in range(chunks):
            relay(1, c)

    nk = 4 * nv
    for c in range(chunks):
        sl = slice(c * SUB, (c + 1) * SUB)
        for v in range(nv):
            x1, x2 = fin[1, c, 0, v], fin[1, c, 1, v]
            rows[c, 4 * v + 2] = ulink[0, v, sl] * x1 + ulink[1, v, sl] * x2
            rows[c, 4 * v + 3] = ulink[2, v, sl] * x1

        def finish(q, carry):
            p = c * SUB + q
            r = jnp.concatenate([rows[c, k, pl.ds(q, 1), :] for k in range(nk)]
                                + [jnp.zeros((32 - nk, width), F32)], axis=0)
            h = r.astype(BF16).astype(F32)
            o = r - h
            right = jnp.concatenate([h, h, o, jnp.zeros((width - 96, width), F32)], axis=0).astype(BF16)
            for v in range(nv):
                add = jnp.dot(lhs[p, v * points:(v + 1) * points, :], right, preferred_element_type=F32)
                obuf[v, p] = obuf[v, p] + add
            return carry

        lax.fori_loop(0, SUB, finish, 0)

    for d in peers:
        donor_copy(d).wait_send()
    for copy in map_copies:
        copy.wait_send()

    @pl.when(l > 0)
    def _():
        down_copy.wait_send()

    @pl.when(l < nl_ - 1)
    def _():
        up_copy.wait_send()

    for side in range(2):
        for c in range(chunks):
            b_copy(side, c).wait_send()

            @pl.when(has_after(side))
            def _():
                chain_copy(side, c).wait_send()


def local(np_, nl_, flow_state, wave_speed, left_eig, right_eig, lower_inverse, upper_inverse, lower_link, upper_link,
          donor_rows, stencil_offsets, donor_weights, block_counts, receptor_rows):
    nv, planes, points, width = flow_state.shape
    chunks = planes // SUB
    cap = donor_rows.shape[3]
    slots = np_ * cap
    vmem = pl.BlockSpec(memory_space=pltpu.VMEM)
    smem = pl.BlockSpec(memory_space=pltpu.SMEM)
    hbm = pl.BlockSpec(memory_space=pltpu.HBM)
    dma = pltpu.SemaphoreType.DMA
    state = (2, chunks, 2, nv, SUB, width)
    return pl.pallas_call(
        functools.partial(kernel, np_, nl_),
        out_shape=pltpu.VMEM(flow_state.shape, F32),
        in_specs=[hbm, hbm, hbm, hbm, smem, smem, vmem, vmem, smem, smem, smem, smem, vmem],
        out_specs=vmem,
        scratch_shapes=[
            pltpu.VMEM((nv, planes, points + 2 * PAD, width), F32),
            pltpu.VMEM((planes, points, width), F32),
            pltpu.VMEM((nv, planes, points, points), F32),
            pltpu.VMEM((nv, planes, points, points), F32),
            pltpu.VMEM((nv, planes, points, 2 * points), BF16),
            pltpu.VMEM((nv, planes, points, 2 * points), BF16),
            pltpu.VMEM((nv, planes, points, width), F32),
            pltpu.VMEM((planes, points, width), F32),
            pltpu.VMEM((planes, nv * points, width), BF16),
            pltpu.VMEM((np_, nv, cap, width), F32),
            pltpu.VMEM((np_, nv, cap, width), F32),
            pltpu.VMEM((2 * slots, (nv + 1) * width), BF16),
            pltpu.VMEM((2, 2, nv, planes, width), F32),
            pltpu.VMEM((2, 2, nv, planes, width), F32),
            pltpu.VMEM((4, planes, width), F32),
            pltpu.VMEM((4, nv, planes, width), F32),
            pltpu.VMEM((2, 4, nv, planes, width), F32),
            pltpu.VMEM((2, 4, nv, planes, width), F32),
            pltpu.VMEM(state, F32),
            pltpu.VMEM(state, F32),
            pltpu.VMEM(state, F32),
            pltpu.VMEM(state, F32),
            pltpu.VMEM((2, nv, planes, width), F32),
            pltpu.VMEM((2, 2, nv, planes, width), F32),
            pltpu.VMEM((2, 4, nv, planes, width), F32),
            pltpu.VMEM((chunks, 4 * nv, SUB, width), F32),
            dma((4,)), dma((np_,)), dma((np_,)), dma((1,)), dma((2,)), dma((2,)), dma((2,)), dma((2,)),
            dma((2, chunks)), dma((2, chunks)), dma((2, chunks)), dma((2, chunks)),
        ],
        compiler_params=pltpu.CompilerParams(
            collective_id=0, has_side_effects=True, vmem_limit_bytes=54 * 1024 * 1024),
    )(flow_state, wave_speed, lower_inverse, upper_inverse, left_eig, right_eig,
      lower_link.reshape(lower_link.shape[:3] + (width,)), upper_link.reshape(upper_link.shape[:3] + (width,)),
      donor_rows, stencil_offsets, donor_weights, jnp.transpose(block_counts, (1, 2, 0)), receptor_rows)


def solution(mesh):
    in_specs = (
        P(None, "plane", "line", None),
        P("plane", "line", None),
        P(),
        P(),
        P(None, "plane", "line", None),
        P(None, "plane", "line", None),
        P(None, None, "plane", "line", None),
        P(None, None, "plane", "line", None),
        P("plane", "line", None, None),
        P("plane", "line", None, None),
        P(None, "plane", "line", None, None),
        P(None, "line", "plane"),
        P("plane", "line", None, None),
    )
    out_specs = P(None, "plane", "line", None)
    body = functools.partial(local, mesh.shape["plane"], mesh.shape["line"])
    return jax.shard_map(body, mesh=mesh, in_specs=in_specs, out_specs=out_specs, check_vma=False)
```
